32 devices in a mesh: row: 8 (over z, core), col: 4 (over y, x).
Axes of the slice: x: 2, y: 2, z: 4, core: 2. Of those that a mesh axis runs over, the one named last changes fastest.
Arguments:
- ladder_ints: float32 [4928, 4928], P('row', 'col'), may hold values from -0.078125 to 0.078125
- amplitudes: float32 [4928, 1024], P('row', 'col'), may hold values from -6 to 6
- phase_map: int32 [8], replicated, may hold values from 0 to 7, each once
Outputs:
- ladder_term: float32 [4928, 1024], P('row', 'col')
The draws below stay inside these ranges and needn't reach their ends.
Inputs may be any that keep to these rules, and one draw needn't show every extreme that they name: `phase_map`: each phase appears once.
All inputs are finite; a program needn't handle non-finite values.
Results may differ from the reference program's by a relative error of at most 0.000078.
Values sent between devices are 32-bit elements; how exact they have to be, the bound alone decides.
A program may use at most 320 MiB of HBM per device.

```python
import jax
import jax.numpy as jnp
from jax import lax

PAIRS = 4928
OCC_PAIRS = 1024
PHASES = 8
N_ROW = 8


def shard_levels(own_key, extent, shards, low, top_value):
    factor_of, own = 1.0, jax.random.fold_in(own_key, 6)
    for axis_at, shards_of in shards:
        draws = jnp.exp(jax.random.uniform(jax.random.fold_in(own, axis_at), (shards_of,), jnp.float32, low / len(shards), top_value / len(shards)))
        factor_of = factor_of * jnp.repeat(draws, extent[axis_at] // shards_of).reshape([-1 if axis == axis_at else 1 for axis in range(len(extent))])
    return factor_of


def gaussian(key, dims, scale, limit, split=(), kind=jnp.bfloat16):
    array = jax.random.normal(key, dims, jnp.float32) * scale
    if len(split) > 0:
        array = shard_levels(key, dims, split, -0.22, 0.18) * array
    return jnp.clip(array, min=-limit, max=limit).astype(kind)


def setup_inputs(seed: int = 0) -> dict:
    streams_of = jax.random.split(jax.random.key(seed), 4)
    ladder_ints = gaussian(streams_of[0], (PAIRS, PAIRS), PAIRS ** -0.5, 0.078125, ((0, 8), (1, 4)), jnp.float32)
    amplitudes = gaussian(streams_of[1], (PAIRS, OCC_PAIRS), 1.0, 6.0, ((0, 8), (1, 4)), jnp.float32)
    phase_map = jax.random.permutation(streams_of[2], N_ROW).astype(jnp.int32)
    return {"ladder_ints": ladder_ints, "amplitudes": amplitudes, "phase_map": phase_map}


def reference(ladder_ints, amplitudes, phase_map):
    block = PAIRS // PHASES
    inverse = jnp.zeros((PHASES,), jnp.int32).at[phase_map.astype(jnp.int32)].set(jnp.arange(PHASES, dtype=jnp.int32))
    shaped = amplitudes.reshape(PHASES, block, OCC_PAIRS)
    by_phase = jnp.take(shaped, inverse, axis=0)
    ordered = jnp.transpose(by_phase, (1, 0, 2)).reshape(PAIRS, OCC_PAIRS)
    return jnp.dot(ladder_ints, ordered, precision=lax.Precision.HIGHEST, preferred_element_type=jnp.float32)
```

```python
import functools

import jax
import jax.numpy as jnp
from jax import lax
from jax.experimental import pallas as pl
from jax.experimental.pallas import tpu as pltpu
from jax.sharding import PartitionSpec as P

LANES = 128
GROUP = 256
MESH = pl.DeviceIdType.MESH


def flipped(index, mask, size):
    value, bit = 0, 1
    while bit < size:
        value = value + bit * (((index // bit) % 2 + (mask // bit) % 2) % 2)
        bit *= 2
    return value


def split(value):
    high = value.astype(jnp.bfloat16)
    return high, (value - high.astype(jnp.float32)).astype(jnp.bfloat16)


def kernel(
    n_row, n_col, halves, phase_ref, v_hbm, a_ref, out_ref,
    v_buf, v_high, v_low, perm, t_cat, blocks, partial, arrived,
    v_sem, block_sem, spread_sem, core_sem, up_sem, down_sem, partial_send, partial_recv,
):
    row, col = lax.axis_index("row"), lax.axis_index("col")
    line = n_row // 2
    chip, core = row // 2, row % 2
    other = chip * 2 + (1 - core)
    up, down = row + 2, row - 2
    has_up, has_down = chip < line - 1, chip > 0
    chunks = n_col * halves
    away = chunks - halves
    rows_each = blocks.shape[2]
    tiles, tile, depth = v_high.shape
    width = v_hbm.shape[1]
    per_group = GROUP // n_row

    def chunk_owner(t):
        return flipped(col, n_col - 1 - t // halves, n_col)

    def load_v(at):
        return pltpu.make_async_copy(v_hbm.at[pl.ds(at * tile, tile)], v_buf, v_sem)

    load_v(0).start()

    barrier = pltpu.get_barrier_semaphore()
    for mask in range(1, n_col):
        pl.semaphore_signal(
            barrier, inc=1, device_id=(row, flipped(col, mask, n_col)), device_id_type=MESH
        )
    pl.semaphore_signal(barrier, inc=1, device_id=(other, col), device_id_type=MESH)

    @pl.when(has_up)
    def _():
        pl.semaphore_signal(barrier, inc=1, device_id=(up, col), device_id_type=MESH)

    @pl.when(has_down)
    def _():
        pl.semaphore_signal(barrier, inc=1, device_id=(down, col), device_id_type=MESH)

    pl.semaphore_wait(barrier, n_col + has_up.astype(jnp.int32) + has_down.astype(jnp.int32))

    def spread(t):
        peer = chunk_owner(t)
        return pltpu.make_async_remote_copy(
            src_ref=a_ref.at[peer, t % halves],
            dst_ref=blocks.at[t, row],
            send_sem=spread_sem.at[t],
            recv_sem=block_sem.at[t, row],
            device_id=(row, peer),
            device_id_type=MESH,
        )

    def keep(t):
        return pltpu.make_async_copy(
            a_ref.at[col, t % halves], blocks.at[t, row], block_sem.at[t, row]
        )

    for t in range(away):
        spread(t).start()
    for t in range(away, chunks):
        keep(t).start()

    lane = lax.broadcasted_iota(jnp.int32, (GROUP, GROUP), 1)
    wanted = (lane % per_group) * n_row
    owner = lane // per_group
    for r in range(n_row):
        wanted = wanted + jnp.where(owner == r, phase_ref[r], 0)
    source = lax.broadcasted_iota(jnp.int32, (GROUP, GROUP), 0)
    perm[...] = jnp.where(source == wanted, 1.0, 0.0).astype(jnp.bfloat16)
    t_cat[...] = jnp.zeros_like(t_cat)

    def pass_on(t, block, sem, target):
        pltpu.make_async_remote_copy(
            src_ref=blocks.at[t, block],
            dst_ref=blocks.at[t, block],
            send_sem=sem,
            recv_sem=block_sem.at[t, block],
            device_id=(target, col),
            device_id_type=MESH,
        ).start()

    def await_block(t, block):
        pltpu.make_async_copy(
            blocks.at[t, block], blocks.at[t, block], block_sem.at[t, block]
        ).wait()

    def regroup(at):
        load_v(at).wait()

        def place(columns, kept):
            high, low = split(v_buf[:, columns])
            moves = perm[:kept, :]
            for to, part in ((v_high, high), (v_low, low)):
                moved = jnp.dot(part, moves, preferred_element_type=jnp.float32)
                yield to, moved.astype(jnp.bfloat16)

        full = width // GROUP

        @pl.loop(0, full)
        def _(g):
            columns = pl.ds(pl.multiple_of(g * GROUP, GROUP), GROUP)
            for to, moved in place(columns, GROUP):
                to[at, :, columns] = moved

        if width % GROUP:
            for to, moved in place(pl.ds(full * GROUP, width % GROUP), width % GROUP):
                to[at, :, full * GROUP:] = moved

    def multiply(t):
        @pl.loop(0, n_row)
        def _(r):
            for g in range(depth // GROUP):
                first = g * per_group
                count = min(per_group, rows_each - first)
                high, low = split(blocks[t, r, first:first + count, :])
                at = pl.ds(pl.multiple_of(g * GROUP + r * per_group, per_group), count)
                t_cat[at, :LANES] = high
                t_cat[at, LANES:] = low

        for at in range(tiles):
            both = jnp.dot(v_high[at], t_cat[...], preferred_element_type=jnp.float32)
            rest = jnp.dot(v_low[at], t_cat[:, :LANES], preferred_element_type=jnp.float32)
            partial[t, at * tile:(at + 1) * tile, :] = both[:, :LANES] + (both[:, LANES:] + rest)

    def give(t):
        return pltpu.make_async_remote_copy(
            src_ref=partial.at[t],
            dst_ref=arrived.at[t],
            send_sem=partial_send.at[t],
            recv_sem=partial_recv.at[t],
            device_id=(row, chunk_owner(t)),
            device_id_type=MESH,
        )

    @pl.loop(0, chunks + line - 1)
    def _(s):
        @pl.when(s < chunks)
        def _():
            await_block(s, row)

            @pl.when(has_up)
            def _():
                pass_on(s, row, up_sem, up)

            @pl.when(has_down)
            def _():
                pass_on(s, row, down_sem, down)

            pass_on(s, row, core_sem, other)

        @pl.when(s == 0)
        def _():
            for at in range(tiles):
                if at:
                    load_v(at).start()
                regroup(at)

        for far in range(1, line):
            t = s - far

            @pl.when((t >= 0) & (t < chunks))
            def _():
                @pl.when(chip >= far)
                def _():
                    block = row - 2 * far
                    await_block(t, block)

                    @pl.when(has_up)
                    def _():
                        pass_on(t, block, up_sem, up)

                    pass_on(t, block, core_sem, other)

                @pl.when(chip + far < line)
                def _():
                    block = row + 2 * far
                    await_block(t, block)

                    @pl.when(has_down)
                    def _():
                        pass_on(t, block, down_sem, down)

                    pass_on(t, block, core_sem, other)

        done = s - (line - 1)

        @pl.when(done >= 0)
        def _():
            for j in range(line):
                await_block(done, j * 2 + (1 - core))
            multiply(done)

            @pl.when(done < away)
            def _():
                give(done).start()

    for t in range(away):
        give(t).wait_recv()
    for h in range(halves):
        total = partial[away + h]
        for t in range(h, away, halves):
            total = total + arrived[t]
        out_ref[:, h * LANES:(h + 1) * LANES] = total

    def await_sent(sem, count):
        sent = blocks.at[:, pl.ds(0, count)]
        pltpu.make_async_copy(sent, sent, sem).wait()

    for t in range(away):
        give(t).wait_send()
        spread(t).wait_send()
    await_sent(core_sem, line)
    for at in range(line - 1):
        @pl.when(chip == at)
        def _():
            await_sent(up_sem, at + 1)

        @pl.when(chip == line - 1 - at)
        def _():
            await_sent(down_sem, at + 1)


def per_device(n_row, n_col, ladder_ints, amplitudes, phase_map):
    rows, width = ladder_ints.shape
    block, own = amplitudes.shape
    rows_each, halves = block // n_col, own // LANES
    chunks = n_col * halves
    depth = -(-width // GROUP) * GROUP
    tile = max(m for m in range(8, 641, 8) if rows % m == 0)
    tiles = rows // tile
    pieces = amplitudes.reshape(n_col, rows_each, halves, LANES).transpose(0, 2, 1, 3)
    dma = pltpu.SemaphoreType.DMA
    return pl.pallas_call(
        functools.partial(kernel, n_row, n_col, halves),
        out_shape=jax.ShapeDtypeStruct((rows, own), jnp.float32),
        in_specs=[
            pl.BlockSpec(memory_space=pltpu.SMEM),
            pl.BlockSpec(memory_space=pl.ANY),
            pl.BlockSpec(memory_space=pltpu.VMEM),
        ],
        out_specs=pl.BlockSpec(memory_space=pltpu.VMEM),
        scratch_shapes=[
            pltpu.VMEM((tile, width), jnp.float32),
            pltpu.VMEM((tiles, tile, depth), jnp.bfloat16),
            pltpu.VMEM((tiles, tile, depth), jnp.bfloat16),
            pltpu.VMEM((GROUP, GROUP), jnp.bfloat16),
            pltpu.VMEM((depth, 2 * LANES), jnp.bfloat16),
            pltpu.VMEM((chunks, n_row, rows_each, LANES), jnp.float32),
            pltpu.VMEM((chunks, rows, LANES), jnp.float32),
            pltpu.VMEM((chunks - halves, rows, LANES), jnp.float32),
            dma,
            dma((chunks, n_row)),
            dma((chunks - halves,)),
            dma,
            dma,
            dma,
            dma((chunks - halves,)),
            dma((chunks - halves,)),
        ],
        compiler_params=pltpu.CompilerParams(
            collective_id=0, has_side_effects=True, vmem_limit_bytes=67043328
        ),
    )(phase_map, ladder_ints, pieces)


def solution(mesh):
    in_specs = (P("row", "col"), P("row", "col"), P())
    out_specs = P("row", "col")
    return jax.shard_map(
        functools.partial(per_device, mesh.shape["row"], mesh.shape["col"]),
        mesh=mesh, in_specs=in_specs, out_specs=out_specs, check_vma=False,
    )
```

```python
import functools

import jax
import jax.numpy as jnp
from jax import lax
from jax.experimental import pallas as pl
from jax.experimental.pallas import tpu as pltpu
from jax.sharding import PartitionSpec as P

LANES = 128
GROUP = 256
LEAD = 1
MESH = pl.DeviceIdType.MESH


def flipped(index, mask, size):
    value, bit = 0, 1
    while bit < size:
        value = value + bit * (((index // bit) % 2 + (mask // bit) % 2) % 2)
        bit *= 2
    return value


def split(value):
    high = value.astype(jnp.bfloat16)
    return high, (value - high.astype(jnp.float32)).astype(jnp.bfloat16)


def kernel(
    n_row, n_col, halves, phase_ref, v_hbm, a_hbm, out_ref,
    v_buf, v_high, v_low, perm, t_cat, a_buf, pieces, blocks, partial, arrived,
    v_sem, a_sem, block_sem, spread_sem, core_sem, up_sem, down_sem, partial_send, partial_recv,
):
    row, col = lax.axis_index("row"), lax.axis_index("col")
    line = n_row // 2
    chip, core = row // 2, row % 2
    other = chip * 2 + (1 - core)
    up, down = row + 2, row - 2
    has_up, has_down = chip < line - 1, chip > 0
    chunks = n_col * halves
    away = chunks - halves
    rows_each = blocks.shape[2]
    tiles, tile, depth = v_high.shape
    width = v_hbm.shape[1]
    per_group = GROUP // n_row

    def chunk_owner(t):
        return flipped(col, n_col - 1 - t // halves, n_col)

    def load_v(at):
        return pltpu.make_async_copy(v_hbm.at[pl.ds(at * tile, tile)], v_buf, v_sem)

    load_a = pltpu.make_async_copy(a_hbm, a_buf, a_sem)
    load_a.start()
    load_v(0).start()

    barrier = pltpu.get_barrier_semaphore()
    for mask in range(1, n_col):
        pl.semaphore_signal(
            barrier, inc=1, device_id=(row, flipped(col, mask, n_col)), device_id_type=MESH
        )
    pl.semaphore_signal(barrier, inc=1, device_id=(other, col), device_id_type=MESH)

    @pl.when(has_up)
    def _():
        pl.semaphore_signal(barrier, inc=1, device_id=(up, col), device_id_type=MESH)

    @pl.when(has_down)
    def _():
        pl.semaphore_signal(barrier, inc=1, device_id=(down, col), device_id_type=MESH)

    load_a.wait()
    for c in range(n_col):
        for h in range(halves):
            pieces[c, h] = a_buf[c * rows_each:(c + 1) * rows_each, h * LANES:(h + 1) * LANES]

    pl.semaphore_wait(barrier, n_col + has_up.astype(jnp.int32) + has_down.astype(jnp.int32))

    def spread(t):
        peer = chunk_owner(t)
        return pltpu.make_async_remote_copy(
            src_ref=pieces.at[peer, t % halves],
            dst_ref=blocks.at[t, row],
            send_sem=spread_sem.at[t],
            recv_sem=block_sem.at[t, row],
            device_id=(row, peer),
            device_id_type=MESH,
        )

    def keep(t):
        return pltpu.make_async_copy(
            pieces.at[col, t % halves], blocks.at[t, row], block_sem.at[t, row]
        )

    def pass_on(t, block, sem, target, source=None):
        pltpu.make_async_remote_copy(
            src_ref=blocks.at[t, block] if source is None else source,
            dst_ref=blocks.at[t, block],
            send_sem=sem,
            recv_sem=block_sem.at[t, block],
            device_id=(target, col),
            device_id_type=MESH,
        ).start()

    def pass_own(t, source=None):
        @pl.when(has_up)
        def _():
            pass_on(t, row, up_sem, up, source)

        @pl.when(has_down)
        def _():
            pass_on(t, row, down_sem, down, source)

        pass_on(t, row, core_sem, other, source)

    for t in range(away):
        spread(t).start()
    for t in range(away, chunks):
        pass_own(t, pieces.at[col, t % halves])
        keep(t).start()

    lane = lax.broadcasted_iota(jnp.int32, (GROUP, GROUP), 1)
    wanted = (lane % per_group) * n_row
    owner = lane // per_group
    for r in range(n_row):
        wanted = wanted + jnp.where(owner == r, phase_ref[r], 0)
    source = lax.broadcasted_iota(jnp.int32, (GROUP, GROUP), 0)
    perm[...] = jnp.where(source == wanted, 1.0, 0.0).astype(jnp.bfloat16)
    t_cat[...] = jnp.zeros_like(t_cat)

    def await_block(t, block):
        pltpu.make_async_copy(
            blocks.at[t, block], blocks.at[t, block], block_sem.at[t, block]
        ).wait()

    def regroup(at):
        load_v(at).wait()

        def place(columns, kept):
            high, low = split(v_buf[:, columns])
            moves = perm[:kept, :]
            for to, part in ((v_high, high), (v_low, low)):
                moved = jnp.dot(part, moves, preferred_element_type=jnp.float32)
                yield to, moved.astype(jnp.bfloat16)

        full = width // GROUP

        @pl.loop(0, full)
        def _(g):
            columns = pl.ds(pl.multiple_of(g * GROUP, GROUP), GROUP)
            for to, moved in place(columns, GROUP):
                to[at, :, columns] = moved

        if width % GROUP:
            for to, moved in place(pl.ds(full * GROUP, width % GROUP), width % GROUP):
                to[at, :, full * GROUP:] = moved

    def multiply(t):
        @pl.loop(0, n_row)
        def _(r):
            for g in range(depth // GROUP):
                first = g * per_group
                count = min(per_group, rows_each - first)
                high, low = split(blocks[t, r, first:first + count, :])
                at = pl.ds(pl.multiple_of(g * GROUP + r * per_group, per_group), count)
                t_cat[at, :LANES] = high
                t_cat[at, LANES:] = low

        for at in range(tiles):
            both = jnp.dot(v_high[at], t_cat[...], preferred_element_type=jnp.float32)
            rest = jnp.dot(v_low[at], t_cat[:, :LANES], preferred_element_type=jnp.float32)
            partial[t, at * tile:(at + 1) * tile, :] = both[:, :LANES] + (both[:, LANES:] + rest)

    def give(t):
        return pltpu.make_async_remote_copy(
            src_ref=partial.at[t],
            dst_ref=arrived.at[t],
            send_sem=partial_send.at[t],
            recv_sem=partial_recv.at[t],
            device_id=(row, chunk_owner(t)),
            device_id_type=MESH,
        )

    @pl.loop(0, chunks + LEAD + line - 1)
    def _(s):
        @pl.when(s < chunks)
        def _():
            await_block(s, row)

        @pl.when(s < away)
        def _():
            pass_own(s)

        @pl.when(s == LEAD)
        def _():
            for at in range(tiles):
                if at:
                    load_v(at).start()
                regroup(at)

        for far in range(1, line):
            t = s - LEAD - far

            @pl.when((t >= 0) & (t < chunks))
            def _():
                @pl.when(chip >= far)
                def _():
                    block = row - 2 * far
                    await_block(t, block)

                    @pl.when(has_up)
                    def _():
                        pass_on(t, block, up_sem, up)

                    pass_on(t, block, core_sem, other)

                @pl.when(chip + far < line)
                def _():
                    block = row + 2 * far
                    await_block(t, block)

                    @pl.when(has_down)
                    def _():
                        pass_on(t, block, down_sem, down)

                    pass_on(t, block, core_sem, other)

        done = s - LEAD - (line - 1)

        @pl.when(done >= 0)
        def _():
            for j in range(line):
                await_block(done, j * 2 + (1 - core))
            multiply(done)

            @pl.when(done < away)
            def _():
                give(done).start()

    for t in range(away):
        give(t).wait_recv()
    for h in range(halves):
        total = partial[away + h]
        for t in range(h, away, halves):
            total = total + arrived[t]
        out_ref[:, h * LANES:(h + 1) * LANES] = total

    def await_sent(sem, count):
        sent = blocks.at[:, pl.ds(0, count)]
        pltpu.make_async_copy(sent, sent, sem).wait()

    for t in range(away):
        give(t).wait_send()
        spread(t).wait_send()
    await_sent(core_sem, line)
    for at in range(line - 1):
        @pl.when(chip == at)
        def _():
            await_sent(up_sem, at + 1)

        @pl.when(chip == line - 1 - at)
        def _():
            await_sent(down_sem, at + 1)


def per_device(n_row, n_col, ladder_ints, amplitudes, phase_map):
    rows, width = ladder_ints.shape
    block, own = amplitudes.shape
    rows_each, halves = block // n_col, own // LANES
    chunks = n_col * halves
    depth = -(-width // GROUP) * GROUP
    tile = max(m for m in range(8, 641, 8) if rows % m == 0)
    tiles = rows // tile
    spare = 4 * rows * own * 5 // 4
    dma = pltpu.SemaphoreType.DMA
    return pl.pallas_call(
        functools.partial(kernel, n_row, n_col, halves),
        out_shape=jax.ShapeDtypeStruct((rows, own), jnp.float32),
        in_specs=[
            pl.BlockSpec(memory_space=pltpu.SMEM),
            pl.BlockSpec(memory_space=pltpu.HBM),
            pl.BlockSpec(memory_space=pltpu.HBM),
        ],
        out_specs=pl.BlockSpec(memory_space=pltpu.VMEM),
        scratch_shapes=[
            pltpu.VMEM((tile, width), jnp.float32),
            pltpu.VMEM((tiles, tile, depth), jnp.bfloat16),
            pltpu.VMEM((tiles, tile, depth), jnp.bfloat16),
            pltpu.VMEM((GROUP, GROUP), jnp.bfloat16),
            pltpu.VMEM((depth, 2 * LANES), jnp.bfloat16),
            pltpu.VMEM((block, own), jnp.float32),
            pltpu.VMEM((n_col, halves, rows_each, LANES), jnp.float32),
            pltpu.VMEM((chunks, n_row, rows_each, LANES), jnp.float32),
            pltpu.VMEM((chunks, rows, LANES), jnp.float32),
            pltpu.VMEM((chunks - halves, rows, LANES), jnp.float32),
            dma,
            dma,
            dma((chunks, n_row)),
            dma((chunks - halves,)),
            dma,
            dma,
            dma,
            dma((chunks - halves,)),
            dma((chunks - halves,)),
        ],
        compiler_params=pltpu.CompilerParams(
            collective_id=0, has_side_effects=True, vmem_limit_bytes=67043328 - spare
        ),
    )(phase_map, ladder_ints, amplitudes)


def solution(mesh):
    in_specs = (P("row", "col"), P("row", "col"), P())
    out_specs = P("row", "col")
    return jax.shard_map(
        functools.partial(per_device, mesh.shape["row"], mesh.shape["col"]),
        mesh=mesh, in_specs=in_specs, out_specs=out_specs, check_vma=False,
    )
```

```python
import functools

import jax
import jax.numpy as jnp
from jax import lax
from jax.experimental import pallas as pl
from jax.experimental.pallas import tpu as pltpu
from jax.sharding import PartitionSpec as P

LANES = 128
GROUP = 256
VMEM = 67043328
LEAD = 0
MESH = pl.DeviceIdType.MESH


def flipped(index, mask, size):
    value, bit = 0, 1
    while bit < size:
        value = value + bit * (((index // bit) % 2 + (mask // bit) % 2) % 2)
        bit *= 2
    return value


def chunk_plan(n_col, halves):
    plan = [(m, h) for m in reversed(range(n_col)) for h in range(halves)]
    plan[2], plan[4] = plan[4], plan[2]
    at = {chunk: t for t, chunk in enumerate(plan)}
    parents = {}
    for t, (mask, half) in enumerate(plan):
        if mask:
            low, high = mask & -mask, 1 << (mask.bit_length() - 1)
            parents[t] = at[mask - (high if half % 2 == 0 else low), half]
    return plan, parents


def split(value):
    high = value.astype(jnp.bfloat16)
    return high, (value - high.astype(jnp.float32)).astype(jnp.bfloat16)


def kernel(
    n_row, n_col, halves, phase_ref, v_hbm, a_hbm, out_ref,
    v_buf, v_high, v_low, perm, t_cat, a_buf, pieces, blocks, partial, arrived,
    v_sem, a_sem, block_sem, spread_sem, core_sem, up_sem, down_sem, partial_send, partial_recv,
):
    row, col = lax.axis_index("row"), lax.axis_index("col")
    line = n_row // 2
    chip, core = row // 2, row % 2
    other = chip * 2 + (1 - core)
    up, down = row + 2, row - 2
    has_up, has_down = chip < line - 1, chip > 0
    chunks = n_col * halves
    away = chunks - halves
    rows_each = blocks.shape[2]
    tiles, tile, depth = v_high.shape
    width = v_hbm.shape[1]
    per_group = GROUP // n_row

    plan, parents = chunk_plan(n_col, halves)

    def chunk_owner(t):
        return flipped(col, plan[t][0], n_col)

    def load_v(at):
        return pltpu.make_async_copy(v_hbm.at[pl.ds(at * tile, tile)], v_buf, v_sem)

    load_a = pltpu.make_async_copy(a_hbm, a_buf, a_sem)
    load_a.start()
    load_v(0).start()

    barrier = pltpu.get_barrier_semaphore()
    for mask in range(1, n_col):
        pl.semaphore_signal(
            barrier, inc=1, device_id=(row, flipped(col, mask, n_col)), device_id_type=MESH
        )
    pl.semaphore_signal(barrier, inc=1, device_id=(other, col), device_id_type=MESH)

    @pl.when(has_up)
    def _():
        pl.semaphore_signal(barrier, inc=1, device_id=(up, col), device_id_type=MESH)

    @pl.when(has_down)
    def _():
        pl.semaphore_signal(barrier, inc=1, device_id=(down, col), device_id_type=MESH)

    load_a.wait()
    for c in range(n_col):
        for h in range(halves):
            pieces[c, h] = a_buf[c * rows_each:(c + 1) * rows_each, h * LANES:(h + 1) * LANES]

    pl.semaphore_wait(barrier, n_col + has_up.astype(jnp.int32) + has_down.astype(jnp.int32))

    def spread(t):
        peer = chunk_owner(t)
        return pltpu.make_async_remote_copy(
            src_ref=pieces.at[peer, plan[t][1]],
            dst_ref=blocks.at[t, row],
            send_sem=spread_sem.at[t],
            recv_sem=block_sem.at[t, row],
            device_id=(row, peer),
            device_id_type=MESH,
        )

    def keep(t):
        return pltpu.make_async_copy(
            pieces.at[col, t - away], blocks.at[t, row], block_sem.at[t, row]
        )

    def pass_on(t, block, sem, target, source=None):
        pltpu.make_async_remote_copy(
            src_ref=blocks.at[t, block] if source is None else source,
            dst_ref=blocks.at[t, block],
            send_sem=sem,
            recv_sem=block_sem.at[t, block],
            device_id=(target, col),
            device_id_type=MESH,
        ).start()

    def pass_own(t, source=None):
        @pl.when(has_up)
        def _():
            pass_on(t, row, up_sem, up, source)

        @pl.when(has_down)
        def _():
            pass_on(t, row, down_sem, down, source)

        pass_on(t, row, core_sem, other, source)

    for t in range(away):
        spread(t).start()
    for t in range(away, chunks):
        pass_own(t, pieces.at[col, t - away])
        keep(t).start()

    lane = lax.broadcasted_iota(jnp.int32, (GROUP, GROUP), 1)
    wanted = (lane % per_group) * n_row
    owner = lane // per_group
    for r in range(n_row):
        wanted = wanted + jnp.where(owner == r, phase_ref[r], 0)
    source = lax.broadcasted_iota(jnp.int32, (GROUP, GROUP), 0)
    perm[...] = jnp.where(source == wanted, 1.0, 0.0).astype(jnp.bfloat16)
    t_cat[...] = jnp.zeros_like(t_cat)

    def await_block(t, block):
        pltpu.make_async_copy(
            blocks.at[t, block], blocks.at[t, block], block_sem.at[t, block]
        ).wait()

    def regroup(at):
        load_v(at).wait()

        def place(columns, kept):
            high, low = split(v_buf[:, columns])
            moves = perm[:kept, :]
            for to, part in ((v_high, high), (v_low, low)):
                moved = jnp.dot(part, moves, preferred_element_type=jnp.float32)
                yield to, moved.astype(jnp.bfloat16)

        full = width // GROUP

        @pl.loop(0, full)
        def _(g):
            columns = pl.ds(pl.multiple_of(g * GROUP, GROUP), GROUP)
            for to, moved in place(columns, GROUP):
                to[at, :, columns] = moved

        if width % GROUP:
            for to, moved in place(pl.ds(full * GROUP, width % GROUP), width % GROUP):
                to[at, :, full * GROUP:] = moved

    def multiply(t):
        @pl.loop(0, n_row)
        def _(r):
            for g in range(depth // GROUP):
                first = g * per_group
                count = min(per_group, rows_each - first)
                high, low = split(blocks[t, r, first:first + count, :])
                at = pl.ds(pl.multiple_of(g * GROUP + r * per_group, per_group), count)
                t_cat[at, :LANES] = high
                t_cat[at, LANES:] = low

        for at in range(tiles):
            both = jnp.dot(v_high[at], t_cat[...], preferred_element_type=jnp.float32)
            rest = jnp.dot(v_low[at], t_cat[:, :LANES], preferred_element_type=jnp.float32)
            partial[t, at * tile:(at + 1) * tile, :] = both[:, :LANES] + (both[:, LANES:] + rest)

    def give(t):
        return pltpu.make_async_remote_copy(
            src_ref=partial.at[t],
            dst_ref=arrived.at[t],
            send_sem=partial_send.at[t],
            recv_sem=partial_recv.at[t],
            device_id=(row, flipped(col, plan[t][0] - plan[parents[t]][0], n_col)),
            device_id_type=MESH,
        )

    def collect(t):
        total = partial[t]
        for child in range(t):
            if parents.get(child) == t:
                give(child).wait_recv()
                total = total + arrived[child]
        return total

    @pl.loop(0, chunks + LEAD + line - 1)
    def _(s):
        @pl.when(s < chunks)
        def _():
            await_block(s, row)

        @pl.when(s < away)
        def _():
            pass_own(s)

        @pl.when(s == LEAD)
        def _():
            for at in range(tiles):
                if at:
                    load_v(at).start()
                regroup(at)

        for far in range(1, line):
            t = s - LEAD - far

            @pl.when((t >= 0) & (t < chunks))
            def _():
                @pl.when(chip >= far)
                def _():
                    block = row - 2 * far
                    await_block(t, block)

                    @pl.when(has_up)
                    def _():
                        pass_on(t, block, up_sem, up)

                    pass_on(t, block, core_sem, other)

                @pl.when(chip + far < line)
                def _():
                    block = row + 2 * far
                    await_block(t, block)

                    @pl.when(has_down)
                    def _():
                        pass_on(t, block, down_sem, down)

                    pass_on(t, block, core_sem, other)

        done = s - LEAD - (line - 1)

        @pl.when(done >= 0)
        def _():
            for j in range(line):
                await_block(done, j * 2 + (1 - core))
            multiply(done)

            for t in range(away):
                @pl.when(done == t)
                def _():
                    if t in parents.values():
                        partial[t] = collect(t)
                    give(t).start()

    for h in range(halves):
        out_ref[:, h * LANES:(h + 1) * LANES] = collect(away + h)

    def await_sent(sem, count):
        sent = blocks.at[:, pl.ds(0, count)]
        pltpu.make_async_copy(sent, sent, sem).wait()

    for t in range(away):
        give(t).wait_send()
        spread(t).wait_send()
    await_sent(core_sem, line)
    for at in range(line - 1):
        @pl.when(chip == at)
        def _():
            await_sent(up_sem, at + 1)

        @pl.when(chip == line - 1 - at)
        def _():
            await_sent(down_sem, at + 1)


def per_device(n_row, n_col, ladder_ints, amplitudes, phase_map):
    rows, width = ladder_ints.shape
    block, own = amplitudes.shape
    rows_each, halves = block // n_col, own // LANES
    chunks = n_col * halves
    depth = -(-width // GROUP) * GROUP
    tile = max(m for m in range(8, 641, 8) if rows % m == 0)
    tiles = rows // tile
    need = 4 * (tile * depth + rows * depth + depth * LANES + 3 * block * own)
    need += 4 * LANES * chunks * (n_row * (rows_each + 8) + 2 * rows)
    spare = max(0, min(4 * rows * own * 18, VMEM - need - (1 << 20)))
    dma = pltpu.SemaphoreType.DMA
    return pl.pallas_call(
        functools.partial(kernel, n_row, n_col, halves),
        out_shape=jax.ShapeDtypeStruct((rows, own), jnp.float32),
        in_specs=[
            pl.BlockSpec(memory_space=pltpu.SMEM),
            pl.BlockSpec(memory_space=pltpu.HBM),
            pl.BlockSpec(memory_space=pltpu.HBM),
        ],
        out_specs=pl.BlockSpec(memory_space=pltpu.VMEM),
        scratch_shapes=[
            pltpu.VMEM((tile, width), jnp.float32),
            pltpu.VMEM((tiles, tile, depth), jnp.bfloat16),
            pltpu.VMEM((tiles, tile, depth), jnp.bfloat16),
            pltpu.VMEM((GROUP, GROUP), jnp.bfloat16),
            pltpu.VMEM((depth, 2 * LANES), jnp.bfloat16),
            pltpu.VMEM((block, own), jnp.float32),
            pltpu.VMEM((n_col, halves, rows_each, LANES), jnp.float32),
            pltpu.VMEM((chunks, n_row, rows_each, LANES), jnp.float32),
            pltpu.VMEM((chunks, rows, LANES), jnp.float32),
            pltpu.VMEM((chunks - halves, rows, LANES), jnp.float32),
            dma,
            dma,
            dma((chunks, n_row)),
            dma((chunks - halves,)),
            dma,
            dma,
            dma,
            dma((chunks - halves,)),
            dma((chunks - halves,)),
        ],
        compiler_params=pltpu.CompilerParams(
            collective_id=0, has_side_effects=True, vmem_limit_bytes=VMEM - spare
        ),
    )(phase_map, ladder_ints, amplitudes)


def solution(mesh):
    in_specs = (P("row", "col"), P("row", "col"), P())
    out_specs = P("row", "col")
    return jax.shard_map(
        functools.partial(per_device, mesh.shape["row"], mesh.shape["col"]),
        mesh=mesh, in_specs=in_specs, out_specs=out_specs, check_vma=False,
    )
```

```python
import functools

import jax
import jax.numpy as jnp
from jax import lax
from jax.experimental import pallas as pl
from jax.experimental.pallas import tpu as pltpu
from jax.sharding import PartitionSpec as P

LANES = 128
GROUP = 256
VMEM = 67043328
LEAD = 0
MESH = pl.DeviceIdType.MESH


def flipped(index, mask, size):
    value, bit = 0, 1
    while bit < size:
        value = value + bit * (((index // bit) % 2 + (mask // bit) % 2) % 2)
        bit *= 2
    return value


def chunk_plan(n_col, halves):
    plan = [(m, h) for m in reversed(range(n_col)) for h in range(halves)]
    plan[2], plan[4] = plan[4], plan[2]
    at = {chunk: t for t, chunk in enumerate(plan)}
    parents = {}
    for t, (mask, half) in enumerate(plan):
        if mask:
            low, high = mask & -mask, 1 << (mask.bit_length() - 1)
            parents[t] = at[mask - (high if half % 2 == 0 else low), half]
    return plan, parents


def split(value):
    high = value.astype(jnp.bfloat16)
    return high, (value - high.astype(jnp.float32)).astype(jnp.bfloat16)


def kernel(
    n_row, n_col, halves, phase_ref, v_hbm, a_hbm, out_ref,
    v_buf, v_high, v_low, perm, t_cat, a_buf, pieces, blocks, partial, arrived,
    v_sem, a_sem, block_sem, spread_sem, core_sem, up_sem, down_sem, partial_send, partial_recv,
):
    row, col = lax.axis_index("row"), lax.axis_index("col")
    line = n_row // 2
    chip, core = row // 2, row % 2
    other = chip * 2 + (1 - core)
    up, down = row + 2, row - 2
    has_up, has_down = chip < line - 1, chip > 0
    chunks = n_col * halves
    away = chunks - halves
    rows_each = blocks.shape[2]
    tiles, tile, depth = v_high.shape
    width = v_hbm.shape[1]
    per_group = GROUP // n_row

    plan, parents = chunk_plan(n_col, halves)

    def chunk_owner(t):
        return flipped(col, plan[t][0], n_col)

    def load_v(at):
        return pltpu.make_async_copy(v_hbm.at[pl.ds(at * tile, tile)], v_buf, v_sem)

    load_a = pltpu.make_async_copy(a_hbm, a_buf, a_sem)
    load_a.start()
    load_v(0).start()

    barrier = pltpu.get_barrier_semaphore()
    for mask in range(1, n_col):
        pl.semaphore_signal(
            barrier, inc=1, device_id=(row, flipped(col, mask, n_col)), device_id_type=MESH
        )
    pl.semaphore_signal(barrier, inc=1, device_id=(other, col), device_id_type=MESH)

    @pl.when(has_up)
    def _():
        pl.semaphore_signal(barrier, inc=1, device_id=(up, col), device_id_type=MESH)

    @pl.when(has_down)
    def _():
        pl.semaphore_signal(barrier, inc=1, device_id=(down, col), device_id_type=MESH)

    load_a.wait()
    for c in range(n_col):
        for h in range(halves):
            pieces[c, h] = a_buf[c * rows_each:(c + 1) * rows_each, h * LANES:(h + 1) * LANES]

    pl.semaphore_wait(barrier, n_col + has_up.astype(jnp.int32) + has_down.astype(jnp.int32))

    def spread(t):
        peer = chunk_owner(t)
        return pltpu.make_async_remote_copy(
            src_ref=pieces.at[peer, plan[t][1]],
            dst_ref=blocks.at[t, row],
            send_sem=spread_sem.at[t],
            recv_sem=block_sem.at[t, row],
            device_id=(row, peer),
            device_id_type=MESH,
        )

    def keep(t):
        return pltpu.make_async_copy(
            pieces.at[col, t - away], blocks.at[t, row], block_sem.at[t, row]
        )

    def pass_on(t, block, sem, target, source=None):
        pltpu.make_async_remote_copy(
            src_ref=blocks.at[t, block] if source is None else source,
            dst_ref=blocks.at[t, block],
            send_sem=sem,
            recv_sem=block_sem.at[t, block],
            device_id=(target, col),
            device_id_type=MESH,
        ).start()

    def pass_own(t, source=None):
        @pl.when(has_up)
        def _():
            pass_on(t, row, up_sem, up, source)

        @pl.when(has_down)
        def _():
            pass_on(t, row, down_sem, down, source)

        pass_on(t, row, core_sem, other, source)

    for t in range(away):
        spread(t).start()
    for t in range(away, chunks):
        pass_own(t, pieces.at[col, t - away])
        keep(t).start()

    lane = lax.broadcasted_iota(jnp.int32, (GROUP, GROUP), 1)
    wanted = (lane % per_group) * n_row
    owner = lane // per_group
    for r in range(n_row):
        wanted = wanted + jnp.where(owner == r, phase_ref[r], 0)
    source = lax.broadcasted_iota(jnp.int32, (GROUP, GROUP), 0)
    perm[...] = jnp.where(source == wanted, 1.0, 0.0).astype(jnp.bfloat16)
    t_cat[...] = jnp.zeros_like(t_cat)

    def await_block(t, block):
        pltpu.make_async_copy(
            blocks.at[t, block], blocks.at[t, block], block_sem.at[t, block]
        ).wait()

    def regroup(at):
        load_v(at).wait()

        def place(columns, kept):
            high, low = split(v_buf[:, columns])
            moves = perm[:kept, :]
            for to, part in ((v_high, high), (v_low, low)):
                moved = jnp.dot(part, moves, preferred_element_type=jnp.float32)
                yield to, moved.astype(jnp.bfloat16)

        full = width // GROUP

        @pl.loop(0, full)
        def _(g):
            columns = pl.ds(pl.multiple_of(g * GROUP, GROUP), GROUP)
            for to, moved in place(columns, GROUP):
                to[at, :, columns] = moved

        if width % GROUP:
            for to, moved in place(pl.ds(full * GROUP, width % GROUP), width % GROUP):
                to[at, :, full * GROUP:] = moved

    def multiply(t):
        @pl.loop(0, n_row)
        def _(r):
            for g in range(depth // GROUP):
                first = g * per_group
                count = min(per_group, rows_each - first)
                high, low = split(blocks[t, r, first:first + count, :])
                at = pl.ds(pl.multiple_of(g * GROUP + r * per_group, per_group), count)
                t_cat[at, :LANES] = high
                t_cat[at, LANES:] = low

        for at in range(tiles):
            both = jnp.dot(v_high[at], t_cat[...], preferred_element_type=jnp.float32)
            rest = jnp.dot(v_low[at], t_cat[:, :LANES], preferred_element_type=jnp.float32)
            partial[t, at * tile:(at + 1) * tile, :] = both[:, :LANES] + (both[:, LANES:] + rest)

    def give(t):
        return pltpu.make_async_remote_copy(
            src_ref=partial.at[t],
            dst_ref=arrived.at[t],
            send_sem=partial_send.at[t],
            recv_sem=partial_recv.at[t],
            device_id=(row, flipped(col, plan[t][0] - plan[parents[t]][0], n_col)),
            device_id_type=MESH,
        )

    def collect(t):
        total = partial[t]
        for child in range(t):
            if parents.get(child) == t:
                give(child).wait_recv()
                total = total + arrived[child]
        return total

    @pl.loop(0, chunks + LEAD + line - 1)
    def _(s):
        @pl.when(s < chunks)
        def _():
            await_block(s, row)

        @pl.when(s < away)
        def _():
            pass_own(s)

        @pl.when(s == 1)
        def _():
            for at in range(tiles):
                if at:
                    load_v(at).start()
                regroup(at)

        for far in range(1, line):
            t = s - LEAD - far

            @pl.when((t >= 0) & (t < chunks))
            def _():
                @pl.when(chip >= far)
                def _():
                    block = row - 2 * far
                    await_block(t, block)

                    @pl.when(has_up)
                    def _():
                        pass_on(t, block, up_sem, up)

                    pass_on(t, block, core_sem, other)

                @pl.when(chip + far < line)
                def _():
                    block = row + 2 * far
                    await_block(t, block)

                    @pl.when(has_down)
                    def _():
                        pass_on(t, block, down_sem, down)

                    pass_on(t, block, core_sem, other)

        done = s - LEAD - (line - 1)

        @pl.when(done >= 0)
        def _():
            for j in range(line):
                await_block(done, j * 2 + (1 - core))
            multiply(done)

            for t in range(away):
                @pl.when(done == t)
                def _():
                    if t in parents.values():
                        partial[t] = collect(t)
                    give(t).start()

    for h in range(halves):
        out_ref[:, h * LANES:(h + 1) * LANES] = collect(away + h)

    def await_sent(sem, count):
        sent = blocks.at[:, pl.ds(0, count)]
        pltpu.make_async_copy(sent, sent, sem).wait()

    for t in range(away):
        give(t).wait_send()
        spread(t).wait_send()
    await_sent(core_sem, line)
    for at in range(line - 1):
        @pl.when(chip == at)
        def _():
            await_sent(up_sem, at + 1)

        @pl.when(chip == line - 1 - at)
        def _():
            await_sent(down_sem, at + 1)


def per_device(n_row, n_col, ladder_ints, amplitudes, phase_map):
    rows, width = ladder_ints.shape
    block, own = amplitudes.shape
    rows_each, halves = block // n_col, own // LANES
    chunks = n_col * halves
    depth = -(-width // GROUP) * GROUP
    tile = max(m for m in range(8, 641, 8) if rows % m == 0)
    tiles = rows // tile
    need = 4 * (tile * depth + rows * depth + depth * LANES + 3 * block * own)
    need += 4 * LANES * chunks * (n_row * (rows_each + 8) + 2 * rows)
    spare = max(0, min(4 * rows * own * 18, VMEM - need - (1 << 20)))
    dma = pltpu.SemaphoreType.DMA
    return pl.pallas_call(
        functools.partial(kernel, n_row, n_col, halves),
        out_shape=jax.ShapeDtypeStruct((rows, own), jnp.float32),
        in_specs=[
            pl.BlockSpec(memory_space=pltpu.SMEM),
            pl.BlockSpec(memory_space=pltpu.HBM),
            pl.BlockSpec(memory_space=pltpu.HBM),
        ],
        out_specs=pl.BlockSpec(memory_space=pltpu.VMEM),
        scratch_shapes=[
            pltpu.VMEM((tile, width), jnp.float32),
            pltpu.VMEM((tiles, tile, depth), jnp.bfloat16),
            pltpu.VMEM((tiles, tile, depth), jnp.bfloat16),
            pltpu.VMEM((GROUP, GROUP), jnp.bfloat16),
            pltpu.VMEM((depth, 2 * LANES), jnp.bfloat16),
            pltpu.VMEM((block, own), jnp.float32),
            pltpu.VMEM((n_col, halves, rows_each, LANES), jnp.float32),
            pltpu.VMEM((chunks, n_row, rows_each, LANES), jnp.float32),
            pltpu.VMEM((chunks, rows, LANES), jnp.float32),
            pltpu.VMEM((chunks - halves, rows, LANES), jnp.float32),
            dma,
            dma,
            dma((chunks, n_row)),
            dma((chunks - halves,)),
            dma,
            dma,
            dma,
            dma((chunks - halves,)),
            dma((chunks - halves,)),
        ],
        compiler_params=pltpu.CompilerParams(
            collective_id=0, has_side_effects=True, vmem_limit_bytes=VMEM - spare
        ),
    )(phase_map, ladder_ints, amplitudes)


def solution(mesh):
    in_specs = (P("row", "col"), P("row", "col"), P())
    out_specs = P("row", "col")
    return jax.shard_map(
        functools.partial(per_device, mesh.shape["row"], mesh.shape["col"]),
        mesh=mesh, in_specs=in_specs, out_specs=out_specs, check_vma=False,
    )
```
